32 devices in a mesh: gx: 4 (over y, x), gy: 2 (over core), gz: 4 (over z).
Axes of the slice: x: 2, y: 2, z: 4, core: 2. Of those that a mesh axis runs over, the one named last changes fastest.
Arguments:
- volume: float32 [512, 128, 512], P('gx', 'gy', 'gz'), may hold values from -6 to 6
Outputs:
- prefix: float32 [512, 128, 512], P('gx', 'gy', 'gz')
- box_sum: float32 [512, 128, 512], P('gx', 'gy', 'gz')
The draws below stay inside these ranges and needn't reach their ends.
All inputs are finite; a program needn't handle non-finite values.
Results may differ from the reference program's by a relative error of at most 0.00055.
Values sent between devices are 32-bit elements; how exact they have to be, the bound alone decides.
A program may use at most 128 MiB of HBM per device.

```python
import math
import jax
import jax.numpy as jnp

NX = 512
NY = 128
NZ = 512


def level_of(own_key, shape, split, least, high):
    factor_of = 1.0
    for axis_at, shards_of in split:
        draws = jax.random.uniform(jax.random.fold_in(jax.random.fold_in(own_key, 6), axis_at), (shards_of,), jnp.float32, least / len(split), high / len(split))
        factor_of = factor_of * jnp.repeat(jnp.exp(draws), shape[axis_at] // shards_of).reshape((-1,) + (1,) * (len(shape) - 1 - axis_at))
    return factor_of


def normal_values(stream_key, dims, deviation, bound, pieces=(), dtype=jnp.bfloat16):
    result = jax.random.normal(stream_key, dims, jnp.float32) * deviation
    if len(pieces) > 0:
        result = level_of(stream_key, dims, pieces, -0.22, 0.18) * result
    return jnp.clip(result, min=-bound, max=bound).astype(dtype)


def setup_inputs(seed: int = 0) -> dict:
    key_of = jax.random.split(jax.random.key(seed), 2)
    volume = normal_values(key_of[0], (NX, NY, NZ), 1.0, 6.0, ((0, 4), (1, 2), (2, 4)), jnp.float32)
    return {"volume": volume}


def reference(volume):
    summed = jnp.cumsum(jnp.cumsum(jnp.cumsum(volume, axis=2), axis=1), axis=0)
    size_x, size_y, size_z = volume.shape
    prefix = summed * jnp.float32(1.0 / math.sqrt(size_x * size_y * size_z))
    padded = jnp.pad(summed, ((3, 0), (3, 0), (3, 0)))
    padded = jnp.pad(padded, ((0, 2), (0, 2), (0, 2)), mode='edge')
    total = jnp.zeros(volume.shape, jnp.float32)
    for first in range(2):
        for second in range(2):
            for third in range(2):
                piece = padded[5 * first:5 * first + size_x, 5 * second:5 * second + size_y, 5 * third:5 * third + size_z]
                if (3 - first - second - third) % 2 == 0:
                    total = total + piece
                else:
                    total = total - piece
    box_sum = total * jnp.float32(1.0 / math.sqrt(125.0))
    return (prefix, box_sum)
```

```python
import functools
import math

import jax
import jax.numpy as jnp
from jax import lax
from jax.experimental import pallas as pl
from jax.experimental.pallas import tpu as pltpu
from jax.sharding import PartitionSpec as P

F32 = jnp.float32
BF16 = jnp.bfloat16
MESH = pl.DeviceIdType.MESH
USED = (0, 2, 3, 4, 5)
PLANES = 16


def split(a, axis):
    hi = a.astype(BF16)
    lo = (a - hi.astype(F32)).astype(BF16)
    return jnp.concatenate([hi, lo], axis=axis)


def source_index(kind, length):
    return {2: length - 2, 3: length - 1, 4: 0, 5: 1}[kind]


def selector(length):
    kind = lax.broadcasted_iota(jnp.int32, (8, length), 0)
    at = lax.broadcasted_iota(jnp.int32, (8, length), 1)
    pick = kind == 0
    for k in (2, 3, 4, 5):
        pick = pick | ((kind == k) & (at == source_index(k, length)))
    one = jnp.where(pick, 1.0, 0.0).astype(BF16)
    return jnp.concatenate([one, one], axis=1)


def z_sources(rows):
    return lax.dot_general(
        selector(rows.shape[1]),
        split(rows, 1),
        (((1,), (1,)), ((), ())),
        preferred_element_type=F32,
    )


def sources_kernel(ny, nz, v_ref, x_ref, y_ref, z_ref, zy_ref, zx_ref, zxy_ref):
    i, steps = pl.program_id(0), pl.num_programs(0)
    nx = steps * PLANES
    blocks = PLANES * ny // 128
    zrows = z_ref.shape[0] // 8

    @pl.when(i == 0)
    def _():
        x_ref[...] = jnp.zeros_like(x_ref)
        y_ref[...] = jnp.zeros_like(y_ref)
        x_ref[4] = v_ref[pl.ds(0, ny), :]
        x_ref[5] = v_ref[pl.ds(ny, ny), :]

    total = v_ref[pl.ds(0, ny), :]
    for x in range(1, PLANES):
        total = total + v_ref[pl.ds(x * ny, ny), :]
    x_ref[0] = x_ref[0] + total
    at = pl.ds(pl.multiple_of(i * PLANES, PLANES), PLANES)
    y_ref[0, at, :] = jnp.sum(v_ref[...].reshape(PLANES, ny, nz), axis=1)
    for k in (2, 3, 4, 5):
        y_ref[k, at, :] = v_ref[pl.ds(source_index(k, ny), PLANES, stride=ny), :]
    found = z_sources(v_ref[...])
    for b in range(blocks):
        z_ref[pl.ds(i * blocks + b, 8, stride=zrows), :] = found[:, b * 128 : (b + 1) * 128]

    @pl.when(i == steps - 1)
    def _():
        x_ref[2] = v_ref[pl.ds((PLANES - 2) * ny, ny), :]
        x_ref[3] = v_ref[pl.ds((PLANES - 1) * ny, ny), :]
        count = y_ref.shape[1] - 8
        planes = x_ref[...]
        y_ref[0, pl.ds(count, 8), :] = jnp.sum(planes, axis=1)
        for k in (2, 3, 4, 5):
            y_ref[k, pl.ds(count, 8), :] = planes[:, source_index(k, ny), :]
        for k in range(8):
            zy_ref[k] = z_sources(y_ref[k, pl.ds(0, count), :])
        pairs = planes.reshape(4, 2 * ny, nz)
        for k in range(4):
            zx_ref[k] = z_sources(pairs[k])
        corner = y_ref[:, pl.ds(count, 8), :].reshape(64, nz)
        zxy_ref[0] = z_sources(jnp.concatenate([corner, jnp.zeros_like(corner)], axis=0))


class Exchange:
    def __init__(self, send, recv):
        self.send, self.recv, self.count = send, recv, 0

    def start(self, axis, shift, src, dst):
        n, me = lax.axis_size(axis), lax.axis_index(axis)
        at = self.count
        self.count += 1
        copy = pltpu.make_async_remote_copy(
            src_ref=src,
            dst_ref=dst,
            send_sem=self.send.at[at],
            recv_sem=self.recv.at[at],
            device_id={axis: lax.rem(me + shift + n, n)},
            device_id_type=MESH,
        )
        sends = (me + shift >= 0) & (me + shift < n)
        receives = (me - shift >= 0) & (me - shift < n)
        pl.when(sends)(copy.start)
        return sends, receives, copy

    def layers(self, axis, src, carry, halo):
        out = []
        n = lax.axis_size(axis)
        if n > 1:
            out.append(self.start(axis, 1, src.at[pl.ds(2, 2)], halo.at[pl.ds(0, 2)]))
            out.append(self.start(axis, -1, src.at[pl.ds(4, 2)], halo.at[pl.ds(2, 2)]))
        for d in range(1, n):
            out.append(self.start(axis, d, src.at[pl.ds(0, 1)], carry.at[pl.ds(d - 1, 1)]))
        return out

    def whole(self, axis, src, slots):
        n = lax.axis_size(axis)
        out = [self.start(axis, d, src, slots.at[d - 1]) for d in range(1, n)]
        if n > 1:
            out.append(self.start(axis, -1, src, slots.at[n - 1]))
        return out


def arrived(copies):
    for _, receives, copy in copies:
        pl.when(receives)(copy.wait_recv)


def sent(copies):
    for sends, _, copy in copies:
        pl.when(sends)(copy.wait_send)


def carry_total(carry, n):
    total = carry[0]
    for d in range(1, n - 1):
        total = total + carry[d]
    return total


def put_layers(out_ref, carry, halo, n):
    out_ref[0] = carry_total(carry, n)
    out_ref[1] = jnp.zeros_like(out_ref[1])
    for k in range(4):
        out_ref[2 + k] = halo[k]
    for k in (6, 7):
        out_ref[k] = jnp.zeros_like(out_ref[k])


def combined(slots, n, kind):
    total = slots[0]
    for d in range(1, n - 1):
        total = total + slots[d]
    zero = jnp.zeros_like(total)
    result = jnp.where(kind == 0, total, zero)
    result = jnp.where((kind == 2) | (kind == 3), slots[0], result)
    return jnp.where((kind == 4) | (kind == 5), slots[n - 1], result)


def exchange_kernel(
    x_in, y_in, z_in, zy_in, zx_in, zxy_in,
    x_out, y_out, z_out, zy_out, zx_out, zxy_out,
    xc, xh, yc, yh, zc, zh, zyc, zyh, zyk, zxc, zxh, corner_y, corner_x_src, corner_x,
    z1_src, z1, z2_src, z2, send, recv,
):
    sizes = {a: lax.axis_size(a) for a in ("gx", "gy", "gz")}
    nx, ny, nz = sizes["gx"], sizes["gy"], sizes["gz"]
    for ref in (xc, xh, yc, yh, zc, zh, zyc, zyh, zxc, zxh, corner_y, corner_x, z1, z2):
        ref[...] = jnp.zeros_like(ref)
    barrier = pltpu.get_barrier_semaphore()
    for axis, n in sizes.items():
        me = lax.axis_index(axis)
        for d in range(1, n):
            pl.semaphore_signal(
                barrier, inc=1, device_id={axis: lax.rem(me + d, n)}, device_id_type=MESH
            )
    pl.semaphore_wait(barrier, nx + ny + nz - 3)

    ex = Exchange(send, recv)
    to_y = ex.layers("gy", y_in, yc, yh)
    to_y += ex.layers("gy", zy_in, zyc, zyh)
    to_y += ex.whole("gy", zxy_in, corner_y)
    to_x = ex.layers("gx", x_in, xc, xh)
    to_x.append(ex.start("gx", 1, zx_in.at[pl.ds(1, 1)], zxh.at[pl.ds(0, 1)]))
    to_x.append(ex.start("gx", -1, zx_in.at[pl.ds(2, 1)], zxh.at[pl.ds(1, 1)]))
    for d in range(1, nx):
        to_x.append(ex.start("gx", d, zx_in.at[pl.ds(0, 1)], zxc.at[pl.ds(d - 1, 1)]))
    to_z = ex.layers("gz", z_in, zc, zh)

    lane = lax.broadcasted_iota(jnp.int32, (1, 8, 128), 2)
    row = lax.broadcasted_iota(jnp.int32, (1, 8, 128), 1)
    arrived(to_y)
    count = y_in.shape[1] - 8
    put_layers(y_out, yc, yh, ny)
    put_layers(zyk, zyc, zyh, ny)
    z1_src[...] = zyk[...]
    more_z = ex.whole("gz", z1_src, z1)
    corner_x_src[pl.ds(0, 8)] = y_out[:, pl.ds(count, 8), :]
    corner_x_src[pl.ds(8, 1)] = combined(corner_y, ny, lane // 8)
    more_x = ex.whole("gx", corner_x_src, corner_x)

    arrived(to_x)
    put_layers(x_out, xc, xh, nx)
    z2_src[pl.ds(0, 1)] = carry_total(zxc, nx)[None]
    z2_src[pl.ds(1, 2)] = zxh[...]
    z2_src[pl.ds(3, 1)] = jnp.zeros((1, 8, 128), F32)
    arrived(more_x)
    got = corner_x.at[:, pl.ds(0, 8)]
    y_out[:, pl.ds(count, 8), :] = combined(got, nx, row)
    z2_src[pl.ds(4, 1)] = combined(corner_x.at[:, pl.ds(8, 1)], nx, lax.rem(lane, 8))
    last_z = ex.whole("gz", z2_src, z2)

    arrived(to_z)
    put_layers(z_out, zc, zh, nz)
    arrived(more_z)
    zy_out[...] = combined(z1, nz, row)
    arrived(last_z)
    zx_out[...] = combined(z2.at[:, pl.ds(0, 4)], nz, row)
    zxy_out[...] = combined(z2.at[:, pl.ds(4, 1)], nz, row)
    sent(to_y + to_x + to_z + more_z + more_x + last_z)


def z_weights(nz):
    rows = lax.broadcasted_iota(jnp.int32, (nz, nz), 0)
    cols = lax.broadcasted_iota(jnp.int32, (nz, nz), 1)
    lower = jnp.where(rows <= cols, 1.0, 0.0).astype(BF16)
    band = jnp.where(jnp.abs(rows - cols) <= 2, 1.0, 0.0).astype(BF16)
    half = jnp.concatenate([lower, band], axis=1)
    kind = lax.broadcasted_iota(jnp.int32, (8, nz), 0)
    at = lax.broadcasted_iota(jnp.int32, (8, nz), 1)
    add = (kind == 2) & (at == 0)
    add |= (kind == 3) & (at <= 1)
    add |= (kind == 4) & (at >= nz - 2)
    add |= (kind == 5) & (at == nz - 1)
    edge = jnp.concatenate(
        [jnp.where(kind == 0, 1.0, 0.0).astype(BF16), jnp.where(add, 1.0, 0.0).astype(BF16)], axis=1
    )
    return jnp.concatenate([half, half], axis=0), jnp.concatenate([edge, edge], axis=0)


def along_z(rows, edges, w_ref, e_ref):
    main = jnp.dot(split(rows, 1), w_ref[...], preferred_element_type=F32)
    return main + lax.dot_general(
        split(edges, 0), e_ref[...], (((0,), (0,)), ((), ())), preferred_element_type=F32
    )


def final_kernel(
    ny, nz, scale,
    v_ref, x_ref, y_ref, z_ref, zy_ref, zx_ref, zxy_ref, w_ref, e_ref,
    prefix_ref, box_ref,
    grid_z, rows_y, plane_z, run, tall, boxed,
):
    i, steps = pl.program_id(0), pl.num_programs(0)
    count = y_ref.shape[1] - 8
    blocks = PLANES * ny // 128
    zrows = z_ref.shape[0] // 8

    def y_prefix(piece, start):
        row = lax.broadcasted_iota(jnp.int32, (1, 8, nz), 1)
        c = piece.reshape(ny // 8, 8, nz)
        for step in (1, 2, 4):
            c = c + jnp.where(row >= step, pltpu.roll(c, step, 1), 0.0)
        out = []
        for k in range(ny // 8):
            out.append(c[k] + start)
            start = out[-1][7:8]
        return jnp.concatenate(out, axis=0)

    def y_box(slot, piece, before, after):
        tall[slot, pl.ds(8, ny), :] = piece
        tall[slot, pl.ds(6, 1), :] = before[0]
        tall[slot, pl.ds(7, 1), :] = before[1]
        tall[slot, pl.ds(8 + ny, 1), :] = after[0]
        tall[slot, pl.ds(9 + ny, 1), :] = after[1]
        total = piece
        for d in (6, 7, 9, 10):
            total = total + tall[slot, pl.ds(d, ny), :]
        return total

    def row_of(k, x, part):
        return rows_y[k, pl.ds(x, 1), pl.ds(part * nz, nz)]

    @pl.when(i == 0)
    def _():
        for k in USED:
            rows_y[k, pl.ds(0, count), :] = along_z(
                y_ref[k, pl.ds(0, count), :], zy_ref[k], w_ref, e_ref
            )
        corner = along_z(
            y_ref[:, pl.ds(count, 8), :].reshape(64, nz), zxy_ref[0][:, :64], w_ref, e_ref
        )
        rows_y[:, pl.ds(count, 8), :] = corner.reshape(8, 8, 2 * nz)
        edges = jnp.concatenate([zx_ref[k] for k in range(4)], axis=1)
        plane_z[...] = along_z(x_ref[...].reshape(8 * ny, nz), edges, w_ref, e_ref)
        run[...] = y_prefix(plane_z[pl.ds(0, ny), pl.ds(0, nz)], row_of(0, count, 0))
        for k, to in ((2, 0), (3, 1), (4, count + 2), (5, count + 3)):
            boxed[to] = y_box(
                k % 4,
                plane_z[pl.ds(k * ny, ny), pl.ds(nz, nz)],
                [row_of(t, count + k, 1) for t in (2, 3)],
                [row_of(t, count + k, 1) for t in (4, 5)],
            )

    @pl.when(i < steps - 1)
    def _():
        edges = jnp.concatenate(
            [z_ref[pl.ds(i * blocks + b, 8, stride=zrows), :] for b in range(blocks)], axis=1
        )
        grid_z[...] = along_z(v_ref[...], edges, w_ref, e_ref)
        running = run[...]
        here = pl.ds(pl.multiple_of(i * PLANES, PLANES), PLANES)
        starts = rows_y[0, here, pl.ds(0, nz)]
        sides = {t: rows_y[t, here, pl.ds(nz, nz)] for t in (2, 3, 4, 5)}
        for p in range(PLANES):
            x = i * PLANES + p
            at = pl.ds(p * ny, ny)
            running = running + y_prefix(grid_z[at, pl.ds(0, nz)], starts[p : p + 1])
            prefix_ref[at, :] = running * F32(scale)
            boxed[x + 2] = y_box(
                p % 4,
                grid_z[at, pl.ds(nz, nz)],
                [sides[t][p : p + 1] for t in (2, 3)],
                [sides[t][p : p + 1] for t in (4, 5)],
            )
        run[...] = running

    @pl.when(i > 0)
    def _():
        for p in range(PLANES):
            x = (i - 1) * PLANES + p
            total = boxed[x]
            for d in range(1, 5):
                total = total + boxed[x + d]
            box_ref[pl.ds(p * ny, ny), :] = total * F32(1.0 / math.sqrt(125.0))


def fixed(*shape):
    return pl.BlockSpec(shape, lambda i: (0,) * len(shape))


def per_device(volume):
    cx, cy, cz = volume.shape
    nx, ny, nz = (lax.axis_size(a) for a in ("gx", "gy", "gz"))
    steps = cx // PLANES
    rows = PLANES * cy
    zrows = cx * cy // 128
    flat = volume.reshape(cx * cy, cz)

    def of(*shape):
        return jax.ShapeDtypeStruct(shape, F32)

    faces = [(8, cy, cz), (8, cx + 8, cz), (8 * zrows, 128), (8, 8, cx), (4, 8, 2 * cy), (1, 8, 128)]
    x, y, z, zy, zx, zxy = pl.pallas_call(
        functools.partial(sources_kernel, cy, cz),
        grid=(steps,),
        in_specs=[pl.BlockSpec((rows, cz), lambda i: (i, 0))],
        out_specs=[fixed(*s) for s in faces],
        out_shape=[of(*s) for s in faces],
    )(flat)

    z = z.reshape(8, zrows, 128)
    vmem = pl.BlockSpec(memory_space=pltpu.VMEM)
    sent_shapes = [a.shape for a in (x, y, z, zy, zx, zxy)]
    copies = 4 * (nx + ny + nz) + 4
    lx, ly, lz = (max(n - 1, 1) for n in (nx, ny, nz))
    buffers = [
        (lx, cy, cz), (4, cy, cz),
        (ly, cx + 8, cz), (4, cx + 8, cz),
        (lz, zrows, 128), (4, zrows, 128),
        (ly, 8, cx), (4, 8, cx), (8, 8, cx),
        (lx, 8, 128), (2, 8, 128),
        (ny, 1, 8, 128),
        (9, 8, 128), (nx, 9, 8, 128),
        (8, 8, 128), (nz, 8, 8, 128),
        (5, 8, 128), (nz, 5, 8, 128),
    ]
    x, y, z, zy, zx, zxy = pl.pallas_call(
        exchange_kernel,
        in_specs=[vmem] * 6,
        out_specs=[vmem] * 6,
        out_shape=[of(*s) for s in sent_shapes],
        scratch_shapes=[pltpu.VMEM(s, F32) for s in buffers]
        + [pltpu.SemaphoreType.DMA((copies,)), pltpu.SemaphoreType.DMA((copies,))],
        compiler_params=pltpu.CompilerParams(collective_id=0, has_side_effects=True),
    )(x, y, z, zy, zx, zxy)
    z = z.reshape(8 * zrows, 128)

    weights, edge_weights = z_weights(cz)
    scale = 1.0 / math.sqrt(cx * nx * cy * ny * cz * nz)
    prefix, box = pl.pallas_call(
        functools.partial(final_kernel, cy, cz, scale),
        grid=(steps + 1,),
        in_specs=[pl.BlockSpec((rows, cz), lambda i: (jnp.minimum(i, steps - 1), 0))]
        + [fixed(*a.shape) for a in (x, y, z, zy, zx, zxy, weights, edge_weights)],
        out_specs=[
            pl.BlockSpec((rows, cz), lambda i: (jnp.minimum(i, steps - 1), 0)),
            pl.BlockSpec((rows, cz), lambda i: (jnp.maximum(i - 1, 0), 0)),
        ],
        out_shape=[of(cx * cy, cz), of(cx * cy, cz)],
        scratch_shapes=[
            pltpu.VMEM((rows, 2 * cz), F32),
            pltpu.VMEM((8, cx + 8, 2 * cz), F32),
            pltpu.VMEM((8 * cy, 2 * cz), F32),
            pltpu.VMEM((cy, cz), F32),
            pltpu.VMEM((4, cy + 16, cz), F32),
            pltpu.VMEM((cx + 4, cy, cz), F32),
        ],
        compiler_params=pltpu.CompilerParams(vmem_limit_bytes=63 * 1024 * 1024),
    )(flat, x, y, z, zy, zx, zxy, weights, edge_weights)
    return prefix.reshape(cx, cy, cz), box.reshape(cx, cy, cz)


def solution(mesh):
    return jax.shard_map(
        per_device,
        mesh=mesh,
        in_specs=(P("gx", "gy", "gz"),),
        out_specs=(P("gx", "gy", "gz"), P("gx", "gy", "gz")),
        check_vma=False,
    )
```

```python
import functools
import math

import jax
import jax.numpy as jnp
from jax import lax
from jax.experimental import pallas as pl
from jax.experimental.pallas import tpu as pltpu
from jax.sharding import PartitionSpec as P

F32 = jnp.float32
BF16 = jnp.bfloat16
MESH = pl.DeviceIdType.MESH
PLANES = 16


def split(a, axis):
    hi = a.astype(BF16)
    lo = (a - hi.astype(F32)).astype(BF16)
    return jnp.concatenate([hi, lo], axis=axis)


def dot(a, b):
    return jnp.dot(a, b, preferred_element_type=F32)


def dot_t(a, b):
    return lax.dot_general(a, b, (((0,), (0,)), ((), ())), preferred_element_type=F32)


def twice(a):
    one = jnp.where(a, 1.0, 0.0).astype(BF16)
    return jnp.concatenate([one, one], axis=0)


def z_weights(nz):
    rows = lax.broadcasted_iota(jnp.int32, (nz, nz), 0)
    cols = lax.broadcasted_iota(jnp.int32, (nz, nz), 1)
    return twice(rows <= cols), twice(jnp.abs(rows - cols) <= 2)


def edge_weights(nz):
    kind = lax.broadcasted_iota(jnp.int32, (8, 2 * nz), 0)
    lane = lax.broadcasted_iota(jnp.int32, (8, 2 * nz), 1)
    at = lane - nz
    add = (kind == 0) & (lane < nz)
    add |= (kind == 1) & (at == 0)
    add |= (kind == 2) & (at >= 0) & (at <= 1)
    add |= (kind == 3) & (at >= nz - 2)
    add |= (kind == 4) & (at == nz - 1)
    return twice(add)


def face_weights(cy):
    row = lax.broadcasted_iota(jnp.int32, (128, 128), 0)
    col = lax.broadcasted_iota(jnp.int32, (128, 128), 1)
    same = row // cy == col // cy
    r, c = row % cy, col % cy
    return [
        twice(same & (r <= c)),
        twice(same),
        twice(same & (jnp.abs(r - c) <= 2)),
        twice(same & (c + cy - r <= 2)),
        twice(same & (r + cy - c <= 2)),
    ]


def y_prefix(piece, start):
    ny, nz = piece.shape
    row = lax.broadcasted_iota(jnp.int32, (1, 8, nz), 1)
    c = piece.reshape(ny // 8, 8, nz)
    for step in (1, 2, 4):
        c = c + jnp.where(row >= step, pltpu.roll(c, step, 1), 0.0)
    out = []
    for k in range(ny // 8):
        out.append(c[k] + start)
        start = out[-1][7:8]
    return jnp.concatenate(out, axis=0)


def y_box(tall, slot, piece, before, after):
    ny = piece.shape[0]
    tall[slot, pl.ds(8, ny), :] = piece
    tall[slot, pl.ds(6, 1), :] = before[0]
    tall[slot, pl.ds(7, 1), :] = before[1]
    tall[slot, pl.ds(8 + ny, 1), :] = after[0]
    tall[slot, pl.ds(9 + ny, 1), :] = after[1]
    total = piece
    for d in (6, 7, 9, 10):
        total = total + tall[slot, pl.ds(d, ny), :]
    return total


class Exchange:
    def __init__(self, send, recv):
        self.send, self.recv, self.count = send, recv, 0

    def start(self, shifts, src, dst):
        at = self.count
        self.count += 1
        device, sends, receives = {}, True, True
        for axis, d in shifts.items():
            n, me = lax.axis_size(axis), lax.axis_index(axis)
            device[axis] = lax.rem(me + d + n, n)
            sends = (me + d >= 0) & (me + d < n) & sends
            receives = (me - d >= 0) & (me - d < n) & receives
        copy = pltpu.make_async_remote_copy(
            src_ref=src,
            dst_ref=dst,
            send_sem=self.send.at[at],
            recv_sem=self.recv.at[at],
            device_id=device,
            device_id_type=MESH,
        )
        pl.when(sends)(copy.start)
        return sends, receives, copy


def arrived(copies):
    for _, receives, copy in copies:
        pl.when(receives)(copy.wait_recv)


def sent(copies):
    for sends, _, copy in copies:
        pl.when(sends)(copy.wait_send)


def total_of(ref):
    total = ref[0]
    for d in range(1, ref.shape[0]):
        total = total + ref[d]
    return total


def sides(n):
    return ((0, 1), (1, -1)) if n > 1 else ()


def exchange_kernel(
    cx, cy, cz, v_hbm,
    yp_out, yb_out, xk_out, xe_out, zk_out,
    v, g, xsrc, ysrc, zraw, zsrc, xzp, xzb,
    yc, yh, zyc, zyh, xc, xh, zc, zh, xzc, xzh, gyc, gyh, tall,
    load, send, recv,
):
    nx, ny, nz = (lax.axis_size(a) for a in ("gx", "gy", "gz"))
    chunk = PLANES * cy
    steps = cx // PLANES
    arows = cx * cy // 128
    per = arows // steps

    def load_of(i):
        at = pl.ds(pl.multiple_of(i * chunk, chunk), chunk)
        return pltpu.make_async_copy(v_hbm.at[at], v.at[at], load.at[i])

    for i in range(steps):
        load_of(i).start()
    for ref in (yc, yh, zyc, zyh, xc, xh, zc, zh, xzc, xzh):
        ref[...] = jnp.zeros_like(ref)
    barrier = pltpu.get_barrier_semaphore()
    peers = 0
    for shifts in [{"gy": d} for d in range(1, ny)] + [
        {"gx": dx, "gz": dz} for dx in range(nx) for dz in range(nz) if dx or dz
    ]:
        device = {a: lax.rem(lax.axis_index(a) + d, lax.axis_size(a)) for a, d in shifts.items()}
        pl.semaphore_signal(barrier, inc=1, device_id=device, device_id_type=MESH)
        peers += 1

    def sources(i, xsum):
        load_of(i).wait()
        base = pl.multiple_of(i * chunk, chunk)
        here = pl.ds(pl.multiple_of(i * PLANES, PLANES), PLANES)
        for p in range(PLANES):
            xsum = xsum + v[pl.ds(base + p * cy, cy), :]
        ysrc[0, here, :] = jnp.sum(v[pl.ds(base, chunk), :].reshape(PLANES, cy, cz), axis=1)
        for k, j in ((1, cy - 2), (2, cy - 1), (3, 0), (4, 1)):
            ysrc[k, here, :] = v[pl.ds(base + j, PLANES, stride=cy), :]
        for b in range(per):
            t = v[pl.ds(base + b * 128, 128), :].T
            row = pl.ds(i * per + b, 1)
            zraw[0, row, :] = jnp.sum(t, axis=0, keepdims=True)
            for k, z in ((1, cz - 2), (2, cz - 1), (3, 0), (4, 1)):
                zraw[k, row, :] = t[z : z + 1]
        return xsum

    xsum = lax.fori_loop(0, steps, sources, jnp.zeros((cy, cz), F32))
    xsrc[0] = xsum
    pl.semaphore_wait(barrier, peers)

    ex = Exchange(send, recv)
    to_y = []
    for s, d in sides(ny):
        to_y.append(ex.start({"gy": d}, ysrc.at[pl.ds(1 + 2 * s, 2)], yh.at[pl.ds(2 * s, 2)]))
        to_y.append(ex.start({"gy": d}, zraw.at[pl.ds(1, 4)], zyh.at[s]))
    for d in range(1, ny):
        to_y.append(ex.start({"gy": d}, ysrc.at[0], yc.at[d - 1]))
        to_y.append(ex.start({"gy": d}, zraw.at[0], zyc.at[d - 1]))

    lower, band = z_weights(cz)
    both = jnp.concatenate([lower, band], axis=1)

    @pl.loop(0, steps)
    def _(i):
        at = pl.ds(pl.multiple_of(i * chunk, chunk), chunk)
        g[at, :] = dot(split(v[at, :], 1), both)

    w_low, w_one, w_band, w_down, w_up = face_weights(cy)
    arrived(to_y)

    ycar = total_of(yc)
    xsrc[0] = y_prefix(xsum, jnp.sum(ycar, axis=0, keepdims=True))
    for q, x in enumerate((cx - 2, cx - 1, 0, 1)):
        rows = [yh[k, pl.ds(x, 1), :] for k in range(4)]
        xsrc[1 + q] = y_box(tall, q, v[pl.ds(x * cy, cy), :], rows[:2], rows[2:])
    zsrc[0] = dot(split(zraw[0], 1), w_low) + dot(split(total_of(zyc), 1), w_one)

    def flat(a):
        return split(a.reshape(4 * arows, 128), 1)

    faces = dot(flat(zraw[pl.ds(1, 4)]), w_band)
    faces = faces + dot(flat(zyh[0]), w_down) + dot(flat(zyh[1]), w_up)
    zsrc[pl.ds(1, 4)] = faces.reshape(4, arows, 128)
    line = jnp.sum(zsrc[0], axis=0, keepdims=True)
    whole = line
    for p in range(1, 128 // cy):
        whole = whole + pltpu.roll(line, p * cy, 1)
    xzp[...] = jnp.broadcast_to(whole, (8, 128))
    for s, a in ((0, arows - 1), (1, 0)):
        for k in range(4):
            xzb[2 * s + k // 2, pl.ds(k % 2, 1), :] = zsrc[1 + k, pl.ds(a, 1), :]

    rest = []
    for s, d in sides(nz):
        rest.append(ex.start({"gz": d}, zsrc.at[pl.ds(1 + 2 * s, 2)], zh.at[pl.ds(2 * s, 2)]))
    for d in range(1, nz):
        rest.append(ex.start({"gz": d}, zsrc.at[0], zc.at[d - 1]))
    for s, d in sides(nx):
        rest.append(ex.start({"gx": d}, xsrc.at[pl.ds(1 + 2 * s, 2)], xh.at[pl.ds(2 * s, 2)]))
    for d in range(1, nx):
        rest.append(ex.start({"gx": d}, xsrc.at[0], xc.at[d - 1]))
    for s, d in sides(nx):
        for t, e in sides(nz):
            at = 2 * s + t
            rest.append(ex.start({"gx": d, "gz": e}, xzb.at[at], xzh.at[at]))
    for d in range(1, nx):
        for e in range(1, nz):
            at = (d - 1) * (nz - 1) + e - 1
            rest.append(ex.start({"gx": d, "gz": e}, xzp, xzc.at[at]))

    gyc[...] = dot(split(ycar, 1), lower)
    gyh[...] = dot(split(yh[...].reshape(4 * cx, cz), 1), band).reshape(4, cx, cz)

    @pl.loop(0, steps)
    def _(i):
        here = pl.ds(pl.multiple_of(i * PLANES, PLANES), PLANES)
        starts = gyc[here, :]
        ends = [gyh[k, here, :] for k in range(4)]
        for p in range(PLANES):
            at = pl.ds(pl.multiple_of(i * chunk, chunk) + p * cy, cy)
            rows = [e[p : p + 1] for e in ends]
            yp_out[at, :] = y_prefix(g[at, pl.ds(0, cz)], starts[p : p + 1])
            yb_out[at, :] = y_box(tall, p % 4, g[at, pl.ds(cz, cz)], rows[:2], rows[2:])

    arrived(rest)
    xk_out[0] = total_of(xc)
    xk_out[pl.ds(1, 4)] = xh[...]
    zero = jnp.zeros((8, 128), F32)
    row = lax.broadcasted_iota(jnp.int32, (8, 128), 0)
    xe_out[0] = jnp.where(row == 0, total_of(xzc), zero)
    for s in range(2):
        low, high = pltpu.roll(xzh[2 * s], 1, 0), pltpu.roll(xzh[2 * s + 1], 3, 0)
        inside = jnp.where((row == 1) | (row == 2), low, zero)
        xe_out[1 + s] = jnp.where((row == 3) | (row == 4), high, inside)
    zk_out[...] = jnp.zeros_like(zk_out)
    zk_out[0, pl.ds(0, arows), :] = total_of(zc)
    zk_out[pl.ds(1, 4), pl.ds(0, arows), :] = zh[...]
    sent(to_y + rest)


def final_kernel(
    cx, cy, cz, scale, yp, yb, xk, xe, zk, prefix_hbm, box_hbm, mm, prefix, box, psem, bsem
):
    chunk = PLANES * cy
    steps = cx // PLANES
    arows = cx * cy // 128
    per = arows // steps
    pad = zk.shape[0] // 8
    box_scale = F32(1.0 / math.sqrt(125.0))
    edge = edge_weights(cz)
    lower, band = z_weights(cz)

    outer = dot_t(split(jnp.concatenate([xe[0], xe[1], xe[2]], axis=1), 0), edge)
    running = dot(split(xk[0], 1), lower) + outer[:cy, :cz]
    halo = dot(split(xk[pl.ds(1, 4)].reshape(4 * cy, cz), 1), band) + outer[128 : 128 + 4 * cy, cz:]
    halo = [halo[k * cy : (k + 1) * cy] for k in range(4)]

    def put(src, dst, sem):
        copy = pltpu.make_async_copy(src, dst, sem)
        copy.start()
        return copy

    copies = []
    window = halo[:2]
    for i in range(steps):
        slot = i % 2
        tiles = [zk[pl.ds(i * per + b, 8, stride=pad), :] for b in range(per)]
        mm[slot] = dot_t(split(jnp.concatenate(tiles, axis=1), 0), edge)
        for p in range(PLANES):
            x = i * PLANES + p
            at, here = pl.ds(x * cy, cy), pl.ds(p * cy, cy)
            running = running + (yp[at, :] + mm[slot, here, pl.ds(0, cz)])
            prefix[at, :] = running * F32(scale)
            window.append(yb[at, :] + mm[slot, here, pl.ds(cz, cz)])
            if len(window) == 5:
                total = (window[0] + window[1]) + (window[2] + window[3]) + window[4]
                box[pl.ds((x - 2) * cy, cy), :] = total * box_scale
                window = window[1:]
        at = pl.ds(i * chunk, chunk)
        copies.append(put(prefix.at[at], prefix_hbm.at[at], psem.at[i]))
        first = max(i * PLANES - 2, 0)
        at = pl.ds(first * cy, ((i + 1) * PLANES - 2 - first) * cy)
        copies.append(put(box.at[at], box_hbm.at[at], bsem.at[i]))
    for k in (2, 3):
        window.append(halo[k])
        total = (window[0] + window[1]) + (window[2] + window[3]) + window[4]
        box[pl.ds((cx - 4 + k) * cy, cy), :] = total * box_scale
        window = window[1:]
    at = pl.ds((cx - 2) * cy, 2 * cy)
    copies.append(put(box.at[at], box_hbm.at[at], bsem.at[steps]))
    for copy in copies:
        copy.wait()


def per_device(volume):
    cx, cy, cz = volume.shape
    nx, ny, nz = (lax.axis_size(a) for a in ("gx", "gy", "gz"))
    steps = cx // PLANES
    rows = cx * cy
    arows = rows // 128
    lx, ly, lz = (max(n - 1, 1) for n in (nx, ny, nz))
    copies = 4 + 2 * ly + 2 + lz + 2 + lx + 4 + lx * lz
    vmem = pl.BlockSpec(memory_space=pltpu.VMEM)
    hbm = pl.BlockSpec(memory_space=pltpu.HBM)
    flat = pltpu.with_memory_space_constraint(volume.reshape(rows, cz), pltpu.HBM)

    outs = [(rows, cz), (rows, cz), (5, cy, cz), (3, 8, 128), (8, arows + 8, 128)]
    buffers = [
        (rows, cz), (rows, 2 * cz), (5, cy, cz), (5, cx, cz),
        (5, arows, 128), (5, arows, 128), (8, 128), (4, 8, 128),
        (ly, cx, cz), (4, cx, cz), (ly, arows, 128), (2, 4, arows, 128),
        (lx, cy, cz), (4, cy, cz), (lz, arows, 128), (4, arows, 128),
        (lx * lz, 8, 128), (4, 8, 128), (cx, cz), (4, cx, cz), (4, cy + 16, cz),
    ]
    yp, yb, xk, xe, zk = pl.pallas_call(
        functools.partial(exchange_kernel, cx, cy, cz),
        in_specs=[hbm],
        out_specs=[vmem] * len(outs),
        out_shape=[pltpu.VMEM(s, F32) for s in outs],
        scratch_shapes=[pltpu.VMEM(s, F32) for s in buffers]
        + [
            pltpu.SemaphoreType.DMA((steps,)),
            pltpu.SemaphoreType.DMA((copies,)),
            pltpu.SemaphoreType.DMA((copies,)),
        ],
        compiler_params=pltpu.CompilerParams(
            collective_id=0, has_side_effects=True, vmem_limit_bytes=40 * 1024 * 1024
        ),
    )(flat)

    scale = 1.0 / math.sqrt(cx * nx * cy * ny * cz * nz)
    prefix, box = pl.pallas_call(
        functools.partial(final_kernel, cx, cy, cz, scale),
        in_specs=[vmem] * 5,
        out_specs=[hbm] * 2,
        out_shape=[jax.ShapeDtypeStruct((rows, cz), F32)] * 2,
        scratch_shapes=[
            pltpu.VMEM((2, PLANES * cy, 2 * cz), F32),
            pltpu.VMEM((rows, cz), F32),
            pltpu.VMEM((rows, cz), F32),
            pltpu.SemaphoreType.DMA((steps,)),
            pltpu.SemaphoreType.DMA((steps + 1,)),
        ],
        compiler_params=pltpu.CompilerParams(vmem_limit_bytes=40 * 1024 * 1024),
    )(yp, yb, xk, xe, zk.reshape(8 * (arows + 8), 128))
    return prefix.reshape(cx, cy, cz), box.reshape(cx, cy, cz)


def solution(mesh):
    return jax.shard_map(
        per_device,
        mesh=mesh,
        in_specs=(P("gx", "gy", "gz"),),
        out_specs=(P("gx", "gy", "gz"), P("gx", "gy", "gz")),
        check_vma=False,
    )
```

```python
import functools
import math

import jax
import jax.numpy as jnp
from jax import lax
from jax.experimental import pallas as pl
from jax.experimental.pallas import tpu as pltpu
from jax.sharding import PartitionSpec as P

F32 = jnp.float32
BF16 = jnp.bfloat16
MESH = pl.DeviceIdType.MESH
PLANES = 16


def split(a, axis):
    hi = a.astype(BF16)
    lo = (a - hi.astype(F32)).astype(BF16)
    return jnp.concatenate([hi, lo], axis=axis)


def dot(a, b):
    return jnp.dot(a, b, preferred_element_type=F32)


def dot_t(a, b):
    return lax.dot_general(a, b, (((0,), (0,)), ((), ())), preferred_element_type=F32)


def twice(a):
    one = jnp.where(a, 1.0, 0.0).astype(BF16)
    return jnp.concatenate([one, one], axis=0)


def z_weights(nz):
    rows = lax.broadcasted_iota(jnp.int32, (nz, nz), 0)
    cols = lax.broadcasted_iota(jnp.int32, (nz, nz), 1)
    return twice(rows <= cols), twice(jnp.abs(rows - cols) <= 2)


def edge_weights(nz):
    kind = lax.broadcasted_iota(jnp.int32, (8, 2 * nz), 0)
    lane = lax.broadcasted_iota(jnp.int32, (8, 2 * nz), 1)
    at = lane - nz
    add = (kind == 0) & (lane < nz)
    add |= (kind == 1) & (at == 0)
    add |= (kind == 2) & (at >= 0) & (at <= 1)
    add |= (kind == 3) & (at >= nz - 2)
    add |= (kind == 4) & (at == nz - 1)
    return twice(add)


def face_weights(cy):
    row = lax.broadcasted_iota(jnp.int32, (128, 128), 0)
    col = lax.broadcasted_iota(jnp.int32, (128, 128), 1)
    same = row // cy == col // cy
    r, c = row % cy, col % cy
    return [
        twice(same & (r <= c)),
        twice(same),
        twice(same & (jnp.abs(r - c) <= 2)),
        twice(same & (c + cy - r <= 2)),
        twice(same & (r + cy - c <= 2)),
    ]


def y_prefix(piece, start):
    ny, nz = piece.shape
    row = lax.broadcasted_iota(jnp.int32, (1, 8, nz), 1)
    c = piece.reshape(ny // 8, 8, nz)
    for step in (1, 2, 4):
        c = c + jnp.where(row >= step, pltpu.roll(c, step, 1), 0.0)
    out = []
    for k in range(ny // 8):
        out.append(c[k] + start)
        start = out[-1][7:8]
    return jnp.concatenate(out, axis=0)


def y_box(tall, slot, piece, before, after):
    ny = piece.shape[0]
    tall[slot, pl.ds(8, ny), :] = piece
    tall[slot, pl.ds(6, 1), :] = before[0]
    tall[slot, pl.ds(7, 1), :] = before[1]
    tall[slot, pl.ds(8 + ny, 1), :] = after[0]
    tall[slot, pl.ds(9 + ny, 1), :] = after[1]
    total = piece
    for d in (6, 7, 9, 10):
        total = total + tall[slot, pl.ds(d, ny), :]
    return total


class Exchange:
    def __init__(self, send, recv):
        self.send, self.recv, self.count = send, recv, 0

    def start(self, shifts, src, dst, step=0):
        at = self.count
        self.count += 1
        device, sends, receives = {}, True, True
        for axis, d in shifts.items():
            n, me = lax.axis_size(axis), lax.axis_index(axis)
            device[axis] = lax.rem(me + d + n, n)
            sends = (me + d >= 0) & (me + d < n) & sends
            receives = (me - d >= 0) & (me - d < n) & receives
            if step:
                sends &= lax.rem(me, 2 * step) == step - 1
                receives &= lax.rem(me - d + n, 2 * step) == step - 1
        copy = pltpu.make_async_remote_copy(
            src_ref=src,
            dst_ref=dst,
            send_sem=self.send.at[at],
            recv_sem=self.recv.at[at],
            device_id=device,
            device_id_type=MESH,
        )
        pl.when(sends)(copy.start)
        return sends, receives, copy


def arrived(copies):
    for _, receives, copy in copies:
        pl.when(receives)(copy.wait_recv)


def sent(copies):
    for sends, _, copy in copies:
        pl.when(sends)(copy.wait_send)


def total_of(ref, count=None):
    total = ref[0]
    for d in range(1, count or ref.shape[0]):
        total = total + ref[d]
    return total


def doublings(n):
    return [1 << k for k in range((n - 1).bit_length())]


def sides(n):
    return ((0, 1), (1, -1)) if n > 1 else ()


def exchange_kernel(
    cx, cy, cz, v_hbm,
    yp_out, yb_out, xk_out, xe_out, zk_out,
    v, g, xsrc, ysrc, zraw, zsrc, xzp, xzb,
    yc, yh, zyc, zyh, xc, xh, zc, zh, xzc, xzh, q, zfw, qfw, gyc, gyh, tall,
    load, send, recv,
):
    nx, ny, nz = (lax.axis_size(a) for a in ("gx", "gy", "gz"))
    chunk = PLANES * cy
    steps = cx // PLANES
    arows = cx * cy // 128
    per = arows // steps

    def load_of(i):
        at = pl.ds(pl.multiple_of(i * chunk, chunk), chunk)
        return pltpu.make_async_copy(v_hbm.at[at], v.at[at], load.at[i])

    for i in range(steps):
        load_of(i).start()
    for ref in (yc, yh, zyc, zyh, xc, xh, zc, zh, xzc, xzh, q):
        ref[...] = jnp.zeros_like(ref)
    barrier = pltpu.get_barrier_semaphore()
    near = [{"gy": d} for d in range(1, ny)] + [{"gx": d} for d in range(1, nx)]
    near += [{"gz": d} for d in range(1, doublings(nz)[-1] + 1 if nz > 1 else 1)]
    near += [{"gx": d, "gz": e} for _, d in sides(nx) for _, e in sides(nz) if d > 0]
    peers = 0
    for shifts in near:
        for sign in (1, -1):
            there, device = True, {}
            for axis, d in shifts.items():
                to, n = lax.axis_index(axis) + sign * d, lax.axis_size(axis)
                there = (to >= 0) & (to < n) & there
                device[axis] = lax.rem(to + n, n)

            @pl.when(there)
            def _():
                pl.semaphore_signal(barrier, inc=1, device_id=device, device_id_type=MESH)

            peers = peers + there.astype(jnp.int32)

    def sources(i, xsum):
        load_of(i).wait()
        base = pl.multiple_of(i * chunk, chunk)
        here = pl.ds(pl.multiple_of(i * PLANES, PLANES), PLANES)
        for p in range(PLANES):
            xsum = xsum + v[pl.ds(base + p * cy, cy), :]
        ysrc[0, here, :] = jnp.sum(v[pl.ds(base, chunk), :].reshape(PLANES, cy, cz), axis=1)
        for k, j in ((1, cy - 2), (2, cy - 1), (3, 0), (4, 1)):
            ysrc[k, here, :] = v[pl.ds(base + j, PLANES, stride=cy), :]
        for b in range(per):
            t = v[pl.ds(base + b * 128, 128), :].T
            row = pl.ds(i * per + b, 1)
            zraw[0, row, :] = jnp.sum(t, axis=0, keepdims=True)
            for k, z in ((1, cz - 2), (2, cz - 1), (3, 0), (4, 1)):
                zraw[k, row, :] = t[z : z + 1]
        return xsum

    xsum = lax.fori_loop(0, steps, sources, jnp.zeros((cy, cz), F32))
    xsrc[0] = xsum
    pl.semaphore_wait(barrier, peers)

    ex = Exchange(send, recv)
    to_y = []
    for s, d in sides(ny):
        to_y.append(ex.start({"gy": d}, ysrc.at[pl.ds(1 + 2 * s, 2)], yh.at[pl.ds(2 * s, 2)]))
        to_y.append(ex.start({"gy": d}, zraw.at[pl.ds(1, 4)], zyh.at[s]))
    for d in range(1, ny):
        to_y.append(ex.start({"gy": d}, ysrc.at[0], yc.at[d - 1]))
        to_y.append(ex.start({"gy": d}, zraw.at[0], zyc.at[d - 1]))

    lower, band = z_weights(cz)
    both = jnp.concatenate([lower, band], axis=1)

    def along_z(i):
        at = pl.ds(pl.multiple_of(i * chunk, chunk), chunk)
        g[at, :] = dot(split(v[at, :], 1), both)

    early = steps // 2
    pl.loop(0, early)(along_z)
    w_low, w_one, w_band, w_down, w_up = face_weights(cy)
    arrived(to_y)

    ycar = total_of(yc)
    xsrc[0] = y_prefix(xsum, jnp.sum(ycar, axis=0, keepdims=True))
    for k, x in enumerate((cx - 2, cx - 1, 0, 1)):
        rows = [yh[b, pl.ds(x, 1), :] for b in range(4)]
        xsrc[1 + k] = y_box(tall, k, v[pl.ds(x * cy, cy), :], rows[:2], rows[2:])
    zsrc[0] = dot(split(zraw[0], 1), w_low) + dot(split(total_of(zyc), 1), w_one)

    def flat(a):
        return split(a.reshape(4 * arows, 128), 1)

    faces = dot(flat(zraw[pl.ds(1, 4)]), w_band)
    faces = faces + dot(flat(zyh[0]), w_down) + dot(flat(zyh[1]), w_up)
    zsrc[pl.ds(1, 4)] = faces.reshape(4, arows, 128)
    line = jnp.sum(zsrc[0], axis=0, keepdims=True)
    whole = line
    for p in range(1, 128 // cy):
        whole = whole + pltpu.roll(line, p * cy, 1)
    xzp[...] = jnp.broadcast_to(whole, (8, 128))
    for s, a in ((0, arows - 1), (1, 0)):
        for k in range(4):
            xzb[2 * s + k // 2, pl.ds(k % 2, 1), :] = zsrc[1 + k, pl.ds(a, 1), :]

    steps_z = doublings(nz)

    def pass_on(k, src, slots):
        step = steps_z[k]
        return [ex.start({"gz": d}, src, slots.at[k], step) for d in range(1, step + 1)]

    lines = [ex.start({"gx": d}, xzp, xzc.at[d - 1]) for d in range(1, nx)]
    rest, carries, ends = [], [], []
    if steps_z:
        carries.append(pass_on(0, zsrc.at[0], zc))
    for s, d in sides(nz):
        rest.append(ex.start({"gz": d}, zsrc.at[pl.ds(1 + 2 * s, 2)], zh.at[pl.ds(2 * s, 2)]))
    for s, d in sides(nx):
        rest.append(ex.start({"gx": d}, xsrc.at[pl.ds(1 + 2 * s, 2)], xh.at[pl.ds(2 * s, 2)]))
    for d in range(1, nx):
        rest.append(ex.start({"gx": d}, xsrc.at[0], xc.at[d - 1]))
    for s, d in sides(nx):
        for t, e in sides(nz):
            at = 2 * s + t
            rest.append(ex.start({"gx": d, "gz": e}, xzb.at[at], xzh.at[at]))

    def forward_carry(k):
        arrived(carries[-1])
        zfw[k] = zsrc[0] + total_of(zc, k)
        carries.append(pass_on(k, zfw.at[k], zc))

    def forward_line(k):
        arrived(ends[-1] if k else lines)
        qfw[k] = total_of(xzc) + (total_of(q, k) if k else 0.0)
        ends.append(pass_on(k, qfw.at[k], q))

    gyc[...] = dot(split(ycar, 1), lower)
    gyh[...] = dot(split(yh[...].reshape(4 * cx, cz), 1), band).reshape(4, cx, cz)

    def along_y(i):
        here = pl.ds(pl.multiple_of(i * PLANES, PLANES), PLANES)
        starts = gyc[here, :]
        beyond = [gyh[k, here, :] for k in range(4)]
        for p in range(PLANES):
            at = pl.ds(pl.multiple_of(i * chunk, chunk) + p * cy, cy)
            rows = [e[p : p + 1] for e in beyond]
            yp_out[at, :] = y_prefix(g[at, pl.ds(0, cz)], starts[p : p + 1])
            yb_out[at, :] = y_box(tall, p % 4, g[at, pl.ds(cz, cz)], rows[:2], rows[2:])

    work = [functools.partial(pl.loop(early, steps), along_z)]
    work += [functools.partial(pl.loop(i, i + 2), along_y) for i in range(0, steps, 2)]
    jobs = [functools.partial(forward_carry, k) for k in range(1, len(steps_z))]
    jobs += [functools.partial(forward_line, k) for k in range(len(steps_z))]
    while work or jobs:
        if work:
            work.pop(0)()
        if jobs and len(work) < 4:
            jobs.pop(0)()

    arrived(rest + sum(carries[-1:] + ends[-1:], []))
    xk_out[0] = total_of(xc)
    xk_out[pl.ds(1, 4)] = xh[...]
    zero = jnp.zeros((8, 128), F32)
    row = lax.broadcasted_iota(jnp.int32, (8, 128), 0)
    xe_out[0] = jnp.where(row == 0, total_of(q), zero)
    for s in range(2):
        low, high = pltpu.roll(xzh[2 * s], 1, 0), pltpu.roll(xzh[2 * s + 1], 3, 0)
        inside = jnp.where((row == 1) | (row == 2), low, zero)
        xe_out[1 + s] = jnp.where((row == 3) | (row == 4), high, inside)
    zk_out[...] = jnp.zeros_like(zk_out)
    zk_out[0, pl.ds(0, arows), :] = total_of(zc)
    zk_out[pl.ds(1, 4), pl.ds(0, arows), :] = zh[...]
    sent(to_y + lines + rest + sum(carries + ends, []))


def final_kernel(
    cx, cy, cz, scale, yp, yb, xk, xe, zk, prefix_hbm, box_hbm, mm, prefix, box, psem, bsem
):
    chunk = PLANES * cy
    steps = cx // PLANES
    arows = cx * cy // 128
    per = arows // steps
    pad = zk.shape[0] // 8
    box_scale = F32(1.0 / math.sqrt(125.0))
    edge = edge_weights(cz)
    lower, band = z_weights(cz)

    outer = dot_t(split(jnp.concatenate([xe[0], xe[1], xe[2]], axis=1), 0), edge)
    running = dot(split(xk[0], 1), lower) + outer[:cy, :cz]
    halo = dot(split(xk[pl.ds(1, 4)].reshape(4 * cy, cz), 1), band) + outer[128 : 128 + 4 * cy, cz:]
    halo = [halo[k * cy : (k + 1) * cy] for k in range(4)]

    def put(src, dst, sem):
        copy = pltpu.make_async_copy(src, dst, sem)
        copy.start()
        return copy

    copies = []
    window = halo[:2]
    for i in range(steps):
        slot = i % 2
        tiles = [zk[pl.ds(i * per + b, 8, stride=pad), :] for b in range(per)]
        mm[slot] = dot_t(split(jnp.concatenate(tiles, axis=1), 0), edge)
        for p in range(PLANES):
            x = i * PLANES + p
            at, here = pl.ds(x * cy, cy), pl.ds(p * cy, cy)
            running = running + (yp[at, :] + mm[slot, here, pl.ds(0, cz)])
            prefix[at, :] = running * F32(scale)
            window.append(yb[at, :] + mm[slot, here, pl.ds(cz, cz)])
            if len(window) == 5:
                total = (window[0] + window[1]) + (window[2] + window[3]) + window[4]
                box[pl.ds((x - 2) * cy, cy), :] = total * box_scale
                window = window[1:]
        at = pl.ds(i * chunk, chunk)
        copies.append(put(prefix.at[at], prefix_hbm.at[at], psem.at[i]))
        first = max(i * PLANES - 2, 0)
        at = pl.ds(first * cy, ((i + 1) * PLANES - 2 - first) * cy)
        copies.append(put(box.at[at], box_hbm.at[at], bsem.at[i]))
    for k in (2, 3):
        window.append(halo[k])
        total = (window[0] + window[1]) + (window[2] + window[3]) + window[4]
        box[pl.ds((cx - 4 + k) * cy, cy), :] = total * box_scale
        window = window[1:]
    at = pl.ds((cx - 2) * cy, 2 * cy)
    copies.append(put(box.at[at], box_hbm.at[at], bsem.at[steps]))
    for copy in copies:
        copy.wait()


def per_device(volume):
    cx, cy, cz = volume.shape
    nx, ny, nz = (lax.axis_size(a) for a in ("gx", "gy", "gz"))
    steps = cx // PLANES
    rows = cx * cy
    arows = rows // 128
    lx, ly = (max(n - 1, 1) for n in (nx, ny))
    lz = max(len(doublings(nz)), 1)
    copies = 4 + 2 * ly + 2 + 2 + lx + 4 + lx + 2 * nz
    vmem = pl.BlockSpec(memory_space=pltpu.VMEM)
    hbm = pl.BlockSpec(memory_space=pltpu.HBM)
    flat = pltpu.with_memory_space_constraint(volume.reshape(rows, cz), pltpu.HBM)

    outs = [(rows, cz), (rows, cz), (5, cy, cz), (3, 8, 128), (8, arows + 8, 128)]
    buffers = [
        (rows, cz), (rows, 2 * cz), (5, cy, cz), (5, cx, cz),
        (5, arows, 128), (5, arows, 128), (8, 128), (4, 8, 128),
        (ly, cx, cz), (4, cx, cz), (ly, arows, 128), (2, 4, arows, 128),
        (lx, cy, cz), (4, cy, cz), (lz, arows, 128), (4, arows, 128),
        (lx, 8, 128), (4, 8, 128), (lz, 8, 128), (lz, arows, 128), (lz, 8, 128), (cx, cz), (4, cx, cz), (4, cy + 16, cz),
    ]
    yp, yb, xk, xe, zk = pl.pallas_call(
        functools.partial(exchange_kernel, cx, cy, cz),
        in_specs=[hbm],
        out_specs=[vmem] * len(outs),
        out_shape=[pltpu.VMEM(s, F32) for s in outs],
        scratch_shapes=[pltpu.VMEM(s, F32) for s in buffers]
        + [
            pltpu.SemaphoreType.DMA((steps,)),
            pltpu.SemaphoreType.DMA((copies,)),
            pltpu.SemaphoreType.DMA((copies,)),
        ],
        compiler_params=pltpu.CompilerParams(
            collective_id=0, has_side_effects=True, vmem_limit_bytes=40 * 1024 * 1024
        ),
    )(flat)

    scale = 1.0 / math.sqrt(cx * nx * cy * ny * cz * nz)
    prefix, box = pl.pallas_call(
        functools.partial(final_kernel, cx, cy, cz, scale),
        in_specs=[vmem] * 5,
        out_specs=[hbm] * 2,
        out_shape=[jax.ShapeDtypeStruct((rows, cz), F32)] * 2,
        scratch_shapes=[
            pltpu.VMEM((2, PLANES * cy, 2 * cz), F32),
            pltpu.VMEM((rows, cz), F32),
            pltpu.VMEM((rows, cz), F32),
            pltpu.SemaphoreType.DMA((steps,)),
            pltpu.SemaphoreType.DMA((steps + 1,)),
        ],
        compiler_params=pltpu.CompilerParams(vmem_limit_bytes=40 * 1024 * 1024),
    )(yp, yb, xk, xe, zk.reshape(8 * (arows + 8), 128))
    return prefix.reshape(cx, cy, cz), box.reshape(cx, cy, cz)


def solution(mesh):
    return jax.shard_map(
        per_device,
        mesh=mesh,
        in_specs=(P("gx", "gy", "gz"),),
        out_specs=(P("gx", "gy", "gz"), P("gx", "gy", "gz")),
        check_vma=False,
    )
```

```python
import functools
import math

import jax
import jax.numpy as jnp
from jax import lax
from jax.experimental import pallas as pl
from jax.experimental.pallas import tpu as pltpu
from jax.sharding import PartitionSpec as P

F32 = jnp.float32
BF16 = jnp.bfloat16
MESH = pl.DeviceIdType.MESH
PLANES = 16
EARLY = 2


def split(a, axis):
    hi = a.astype(BF16)
    lo = (a - hi.astype(F32)).astype(BF16)
    return jnp.concatenate([hi, lo], axis=axis)


def dot(a, b):
    return jnp.dot(a, b, preferred_element_type=F32)


def dot_t(a, b):
    return lax.dot_general(a, b, (((0,), (0,)), ((), ())), preferred_element_type=F32)


def twice(a):
    one = jnp.where(a, 1.0, 0.0).astype(BF16)
    return jnp.concatenate([one, one], axis=0)


def z_weights(nz):
    rows = lax.broadcasted_iota(jnp.int32, (nz, nz), 0)
    cols = lax.broadcasted_iota(jnp.int32, (nz, nz), 1)
    return twice(rows <= cols), twice(jnp.abs(rows - cols) <= 2)


def edge_weights(nz):
    kind = lax.broadcasted_iota(jnp.int32, (8, 2 * nz), 0)
    lane = lax.broadcasted_iota(jnp.int32, (8, 2 * nz), 1)
    at = lane - nz
    add = (kind == 0) & (lane < nz)
    add |= (kind == 1) & (at == 0)
    add |= (kind == 2) & (at >= 0) & (at <= 1)
    add |= (kind == 3) & (at >= nz - 2)
    add |= (kind == 4) & (at == nz - 1)
    return twice(add)


def face_weights(cy):
    row = lax.broadcasted_iota(jnp.int32, (128, 128), 0)
    col = lax.broadcasted_iota(jnp.int32, (128, 128), 1)
    same = row // cy == col // cy
    r, c = row % cy, col % cy
    return [
        twice(same & (r <= c)),
        twice(same),
        twice(same & (jnp.abs(r - c) <= 2)),
        twice(same & (c + cy - r <= 2)),
        twice(same & (r + cy - c <= 2)),
    ]


def y_prefix(piece, start):
    ny, nz = piece.shape
    row = lax.broadcasted_iota(jnp.int32, (1, 8, nz), 1)
    c = piece.reshape(ny // 8, 8, nz)
    for step in (1, 2, 4):
        c = c + jnp.where(row >= step, pltpu.roll(c, step, 1), 0.0)
    out = []
    for k in range(ny // 8):
        out.append(c[k] + start)
        start = out[-1][7:8]
    return jnp.concatenate(out, axis=0)


def y_box(tall, slot, piece, before, after):
    ny = piece.shape[0]
    tall[slot, pl.ds(8, ny), :] = piece
    tall[slot, pl.ds(6, 1), :] = before[0]
    tall[slot, pl.ds(7, 1), :] = before[1]
    tall[slot, pl.ds(8 + ny, 1), :] = after[0]
    tall[slot, pl.ds(9 + ny, 1), :] = after[1]
    total = piece
    for d in (6, 7, 9, 10):
        total = total + tall[slot, pl.ds(d, ny), :]
    return total


class Exchange:
    def __init__(self, send, recv):
        self.send, self.recv, self.count = send, recv, 0

    def start(self, shifts, src, dst, step=0):
        at = self.count
        self.count += 1
        device, sends, receives = {}, True, True
        for axis, d in shifts.items():
            n, me = lax.axis_size(axis), lax.axis_index(axis)
            device[axis] = lax.rem(me + d + n, n)
            sends = (me + d >= 0) & (me + d < n) & sends
            receives = (me - d >= 0) & (me - d < n) & receives
            if step:
                sends &= lax.rem(me, 2 * step) == step - 1
                receives &= lax.rem(me - d + n, 2 * step) == step - 1
        copy = pltpu.make_async_remote_copy(
            src_ref=src,
            dst_ref=dst,
            send_sem=self.send.at[at],
            recv_sem=self.recv.at[at],
            device_id=device,
            device_id_type=MESH,
        )
        pl.when(sends)(copy.start)
        return sends, receives, copy


def arrived(copies):
    for _, receives, copy in copies:
        pl.when(receives)(copy.wait_recv)


def sent(copies):
    for sends, _, copy in copies:
        pl.when(sends)(copy.wait_send)


def total_of(ref, count=None):
    total = ref[0]
    for d in range(1, count or ref.shape[0]):
        total = total + ref[d]
    return total


def doublings(n):
    return [1 << k for k in range((n - 1).bit_length())]


def sides(n):
    return ((0, 1), (1, -1)) if n > 1 else ()


def exchange_kernel(
    cx, cy, cz, v_hbm,
    yp_out, yb_out, xk_out, xe_out, zk_out,
    v, g, xsrc, ysrc, zraw, zsrc, xzp, xzb,
    yc, yh, zyc, zyh, xc, xh, zc, zh, xzc, xzh, q, zfw, qfw, gyc, gyh, tall, w, fw,
    load, send, recv,
):
    nx, ny, nz = (lax.axis_size(a) for a in ("gx", "gy", "gz"))
    chunk = PLANES * cy
    steps = cx // PLANES
    arows = cx * cy // 128
    per = arows // steps

    def load_of(i):
        at = pl.ds(pl.multiple_of(i * chunk, chunk), chunk)
        return pltpu.make_async_copy(v_hbm.at[at], v.at[at], load.at[i])

    for i in range(steps):
        load_of(i).start()
    for ref in (yc, yh, zyc, zyh, xc, xh, zc, zh, xzc, xzh, q):
        ref[...] = jnp.zeros_like(ref)
    barrier = pltpu.get_barrier_semaphore()
    near = [{"gy": d} for d in range(1, ny)] + [{"gx": d} for d in range(1, nx)]
    near += [{"gz": d} for d in range(1, doublings(nz)[-1] + 1 if nz > 1 else 1)]
    near += [{"gx": d, "gz": e} for _, d in sides(nx) for _, e in sides(nz) if d > 0]
    peers = 0
    for shifts in near:
        for sign in (1, -1):
            there, device = True, {}
            for axis, d in shifts.items():
                to, n = lax.axis_index(axis) + sign * d, lax.axis_size(axis)
                there = (to >= 0) & (to < n) & there
                device[axis] = lax.rem(to + n, n)

            @pl.when(there)
            def _():
                pl.semaphore_signal(barrier, inc=1, device_id=device, device_id_type=MESH)

            peers = peers + there.astype(jnp.int32)

    w[...] = jnp.concatenate(z_weights(cz), axis=1)
    for k, weight in enumerate(face_weights(cy)):
        fw[k] = weight

    def sources(i, xsum):
        load_of(i).wait()
        base = pl.multiple_of(i * chunk, chunk)
        here = pl.ds(pl.multiple_of(i * PLANES, PLANES), PLANES)
        for p in range(PLANES):
            xsum = xsum + v[pl.ds(base + p * cy, cy), :]
        ysrc[0, here, :] = jnp.sum(v[pl.ds(base, chunk), :].reshape(PLANES, cy, cz), axis=1)
        for k, j in ((1, cy - 2), (2, cy - 1), (3, 0), (4, 1)):
            ysrc[k, here, :] = v[pl.ds(base + j, PLANES, stride=cy), :]
        for b in range(per):
            t = v[pl.ds(base + b * 128, 128), :].T
            row = pl.ds(i * per + b, 1)
            zraw[0, row, :] = jnp.sum(t, axis=0, keepdims=True)
            for k, z in ((1, cz - 2), (2, cz - 1), (3, 0), (4, 1)):
                zraw[k, row, :] = t[z : z + 1]
        return xsum

    xsum = lax.fori_loop(0, steps, sources, jnp.zeros((cy, cz), F32))
    xsrc[0] = xsum
    pl.semaphore_wait(barrier, peers)

    ex = Exchange(send, recv)
    to_y = []
    for s, d in sides(ny):
        to_y.append(ex.start({"gy": d}, ysrc.at[pl.ds(1 + 2 * s, 2)], yh.at[pl.ds(2 * s, 2)]))
        to_y.append(ex.start({"gy": d}, zraw.at[pl.ds(1, 4)], zyh.at[s]))
    for d in range(1, ny):
        to_y.append(ex.start({"gy": d}, ysrc.at[0], yc.at[d - 1]))
        to_y.append(ex.start({"gy": d}, zraw.at[0], zyc.at[d - 1]))

    def along_z(i):
        at = pl.ds(pl.multiple_of(i * chunk, chunk), chunk)
        g[at, :] = dot(split(v[at, :], 1), w[...])

    early = EARLY
    pl.loop(0, early)(along_z)
    w_low, w_one, w_band, w_down, w_up = (fw[k] for k in range(5))
    arrived(to_y)

    ycar = total_of(yc)
    zsrc[0] = dot(split(zraw[0], 1), w_low) + dot(split(total_of(zyc), 1), w_one)

    def flat(a):
        return split(a.reshape(4 * arows, 128), 1)

    faces = dot(flat(zraw[pl.ds(1, 4)]), w_band)
    faces = faces + dot(flat(zyh[0]), w_down) + dot(flat(zyh[1]), w_up)
    zsrc[pl.ds(1, 4)] = faces.reshape(4, arows, 128)
    line = jnp.sum(zsrc[0], axis=0, keepdims=True)
    whole = line
    for p in range(1, 128 // cy):
        whole = whole + pltpu.roll(line, p * cy, 1)
    xzp[...] = jnp.broadcast_to(whole, (8, 128))
    for s, a in ((0, arows - 1), (1, 0)):
        for k in range(4):
            xzb[2 * s + k // 2, pl.ds(k % 2, 1), :] = zsrc[1 + k, pl.ds(a, 1), :]

    steps_z = doublings(nz)

    def pass_on(k, src, slots):
        step = steps_z[k]
        return [ex.start({"gz": d}, src, slots.at[k], step) for d in range(1, step + 1)]

    lines = [ex.start({"gx": d}, xzp, xzc.at[d - 1]) for d in range(1, nx)]
    rest, carries, ends = [], [], []
    if steps_z:
        carries.append(pass_on(0, zsrc.at[0], zc))
    for s, d in sides(nz):
        rest.append(ex.start({"gz": d}, zsrc.at[pl.ds(1 + 2 * s, 2)], zh.at[pl.ds(2 * s, 2)]))
    xsrc[0] = y_prefix(xsum, jnp.sum(ycar, axis=0, keepdims=True))
    for k, x in enumerate((cx - 2, cx - 1, 0, 1)):
        rows = [yh[b, pl.ds(x, 1), :] for b in range(4)]
        xsrc[1 + k] = y_box(tall, k, v[pl.ds(x * cy, cy), :], rows[:2], rows[2:])
    for s, d in sides(nx):
        rest.append(ex.start({"gx": d}, xsrc.at[pl.ds(1 + 2 * s, 2)], xh.at[pl.ds(2 * s, 2)]))
    for d in range(1, nx):
        rest.append(ex.start({"gx": d}, xsrc.at[0], xc.at[d - 1]))
    for s, d in sides(nx):
        for t, e in sides(nz):
            at = 2 * s + t
            rest.append(ex.start({"gx": d, "gz": e}, xzb.at[at], xzh.at[at]))

    def forward_carry(k):
        arrived(carries[-1])
        zfw[k] = zsrc[0] + total_of(zc, k)
        carries.append(pass_on(k, zfw.at[k], zc))

    def forward_line(k):
        arrived(ends[-1] if k else lines)
        qfw[k] = total_of(xzc) + (total_of(q, k) if k else 0.0)
        ends.append(pass_on(k, qfw.at[k], q))

    gyc[...] = dot(split(ycar, 1), w[:, pl.ds(0, cz)])
    gyh[...] = dot(split(yh[...].reshape(4 * cx, cz), 1), w[:, pl.ds(cz, cz)]).reshape(4, cx, cz)

    def along_y(i):
        here = pl.ds(pl.multiple_of(i * PLANES, PLANES), PLANES)
        starts = gyc[here, :]
        beyond = [gyh[k, here, :] for k in range(4)]
        for p in range(PLANES):
            at = pl.ds(pl.multiple_of(i * chunk, chunk) + p * cy, cy)
            rows = [e[p : p + 1] for e in beyond]
            yp_out[at, :] = y_prefix(g[at, pl.ds(0, cz)], starts[p : p + 1])
            yb_out[at, :] = y_box(tall, p % 4, g[at, pl.ds(cz, cz)], rows[:2], rows[2:])

    work = [functools.partial(pl.loop(early, steps), along_z)]
    work += [functools.partial(pl.loop(i, i + 2), along_y) for i in range(0, steps, 2)]
    jobs = [functools.partial(forward_carry, k) for k in range(1, len(steps_z))]
    jobs += [functools.partial(forward_line, k) for k in range(len(steps_z))]
    while work or jobs:
        if work:
            work.pop(0)()
        if jobs and len(work) < 4:
            jobs.pop(0)()

    arrived(rest + sum(carries[-1:] + ends[-1:], []))
    xk_out[0] = total_of(xc)
    xk_out[pl.ds(1, 4)] = xh[...]
    zero = jnp.zeros((8, 128), F32)
    row = lax.broadcasted_iota(jnp.int32, (8, 128), 0)
    xe_out[0] = jnp.where(row == 0, total_of(q), zero)
    for s in range(2):
        low, high = pltpu.roll(xzh[2 * s], 1, 0), pltpu.roll(xzh[2 * s + 1], 3, 0)
        inside = jnp.where((row == 1) | (row == 2), low, zero)
        xe_out[1 + s] = jnp.where((row == 3) | (row == 4), high, inside)
    zk_out[...] = jnp.zeros_like(zk_out)
    zk_out[0, pl.ds(0, arows), :] = total_of(zc)
    zk_out[pl.ds(1, 4), pl.ds(0, arows), :] = zh[...]
    sent(to_y + lines + rest + sum(carries + ends, []))


def final_kernel(
    cx, cy, cz, scale, yp, yb, xk, xe, zk, prefix_hbm, box_hbm, mm, prefix, box, psem, bsem
):
    chunk = PLANES * cy
    steps = cx // PLANES
    arows = cx * cy // 128
    per = arows // steps
    pad = zk.shape[0] // 8
    box_scale = F32(1.0 / math.sqrt(125.0))
    edge = edge_weights(cz)
    lower, band = z_weights(cz)

    outer = dot_t(split(jnp.concatenate([xe[0], xe[1], xe[2]], axis=1), 0), edge)
    running = dot(split(xk[0], 1), lower) + outer[:cy, :cz]
    halo = dot(split(xk[pl.ds(1, 4)].reshape(4 * cy, cz), 1), band) + outer[128 : 128 + 4 * cy, cz:]
    halo = [halo[k * cy : (k + 1) * cy] for k in range(4)]

    def put(src, dst, sem):
        copy = pltpu.make_async_copy(src, dst, sem)
        copy.start()
        return copy

    copies = []
    window = halo[:2]
    for i in range(steps):
        slot = i % 2
        tiles = [zk[pl.ds(i * per + b, 8, stride=pad), :] for b in range(per)]
        mm[slot] = dot_t(split(jnp.concatenate(tiles, axis=1), 0), edge)
        for p in range(PLANES):
            x = i * PLANES + p
            at, here = pl.ds(x * cy, cy), pl.ds(p * cy, cy)
            running = running + (yp[at, :] + mm[slot, here, pl.ds(0, cz)])
            prefix[at, :] = running * F32(scale)
            window.append(yb[at, :] + mm[slot, here, pl.ds(cz, cz)])
            if len(window) == 5:
                total = (window[0] + window[1]) + (window[2] + window[3]) + window[4]
                box[pl.ds((x - 2) * cy, cy), :] = total * box_scale
                window = window[1:]
        at = pl.ds(i * chunk, chunk)
        copies.append(put(prefix.at[at], prefix_hbm.at[at], psem.at[i]))
        first = max(i * PLANES - 2, 0)
        at = pl.ds(first * cy, ((i + 1) * PLANES - 2 - first) * cy)
        copies.append(put(box.at[at], box_hbm.at[at], bsem.at[i]))
    for k in (2, 3):
        window.append(halo[k])
        total = (window[0] + window[1]) + (window[2] + window[3]) + window[4]
        box[pl.ds((cx - 4 + k) * cy, cy), :] = total * box_scale
        window = window[1:]
    at = pl.ds((cx - 2) * cy, 2 * cy)
    copies.append(put(box.at[at], box_hbm.at[at], bsem.at[steps]))
    for copy in copies:
        copy.wait()


def per_device(volume):
    cx, cy, cz = volume.shape
    nx, ny, nz = (lax.axis_size(a) for a in ("gx", "gy", "gz"))
    steps = cx // PLANES
    rows = cx * cy
    arows = rows // 128
    lx, ly = (max(n - 1, 1) for n in (nx, ny))
    lz = max(len(doublings(nz)), 1)
    copies = 4 + 2 * ly + 2 + 2 + lx + 4 + lx + 2 * nz
    vmem = pl.BlockSpec(memory_space=pltpu.VMEM)
    hbm = pl.BlockSpec(memory_space=pltpu.HBM)
    flat = pltpu.with_memory_space_constraint(volume.reshape(rows, cz), pltpu.HBM)

    outs = [(rows, cz), (rows, cz), (5, cy, cz), (3, 8, 128), (8, arows + 8, 128)]
    buffers = [
        (rows, cz), (rows, 2 * cz), (5, cy, cz), (5, cx, cz),
        (5, arows, 128), (5, arows, 128), (8, 128), (4, 8, 128),
        (ly, cx, cz), (4, cx, cz), (ly, arows, 128), (2, 4, arows, 128),
        (lx, cy, cz), (4, cy, cz), (lz, arows, 128), (4, arows, 128),
        (lx, 8, 128), (4, 8, 128), (lz, 8, 128), (lz, arows, 128), (lz, 8, 128), (cx, cz), (4, cx, cz), (4, cy + 16, cz),
    ]
    yp, yb, xk, xe, zk = pl.pallas_call(
        functools.partial(exchange_kernel, cx, cy, cz),
        in_specs=[hbm],
        out_specs=[vmem] * len(outs),
        out_shape=[pltpu.VMEM(s, F32) for s in outs],
        scratch_shapes=[pltpu.VMEM(s, F32) for s in buffers]
        + [
            pltpu.VMEM((2 * cz, 2 * cz), BF16),
            pltpu.VMEM((5, 256, 128), BF16),
            pltpu.SemaphoreType.DMA((steps,)),
            pltpu.SemaphoreType.DMA((copies,)),
            pltpu.SemaphoreType.DMA((copies,)),
        ],
        compiler_params=pltpu.CompilerParams(
            collective_id=0, has_side_effects=True, vmem_limit_bytes=40 * 1024 * 1024
        ),
    )(flat)

    scale = 1.0 / math.sqrt(cx * nx * cy * ny * cz * nz)
    prefix, box = pl.pallas_call(
        functools.partial(final_kernel, cx, cy, cz, scale),
        in_specs=[vmem] * 5,
        out_specs=[hbm] * 2,
        out_shape=[jax.ShapeDtypeStruct((rows, cz), F32)] * 2,
        scratch_shapes=[
            pltpu.VMEM((2, PLANES * cy, 2 * cz), F32),
            pltpu.VMEM((rows, cz), F32),
            pltpu.VMEM((rows, cz), F32),
            pltpu.SemaphoreType.DMA((steps,)),
            pltpu.SemaphoreType.DMA((steps + 1,)),
        ],
        compiler_params=pltpu.CompilerParams(vmem_limit_bytes=40 * 1024 * 1024),
    )(yp, yb, xk, xe, zk.reshape(8 * (arows + 8), 128))
    return prefix.reshape(cx, cy, cz), box.reshape(cx, cy, cz)


def solution(mesh):
    return jax.shard_map(
        per_device,
        mesh=mesh,
        in_specs=(P("gx", "gy", "gz"),),
        out_specs=(P("gx", "gy", "gz"), P("gx", "gy", "gz")),
        check_vma=False,
    )
```

```python
import functools
import math

import jax
import jax.numpy as jnp
from jax import lax
from jax.experimental import pallas as pl
from jax.experimental.pallas import tpu as pltpu
from jax.sharding import PartitionSpec as P

F32 = jnp.float32
BF16 = jnp.bfloat16
MESH = pl.DeviceIdType.MESH
PLANES = 16
EARLY = 2


def split(a, axis):
    hi = a.astype(BF16)
    lo = (a - hi.astype(F32)).astype(BF16)
    return jnp.concatenate([hi, lo], axis=axis)


def dot(a, b):
    return jnp.dot(a, b, preferred_element_type=F32)


def dot_t(a, b):
    return lax.dot_general(a, b, (((0,), (0,)), ((), ())), preferred_element_type=F32)


def twice(a):
    one = jnp.where(a, 1.0, 0.0).astype(BF16)
    return jnp.concatenate([one, one], axis=0)


def z_weights(nz):
    rows = lax.broadcasted_iota(jnp.int32, (nz, nz), 0)
    cols = lax.broadcasted_iota(jnp.int32, (nz, nz), 1)
    return twice(rows <= cols), twice(jnp.abs(rows - cols) <= 2)


def edge_weights(nz):
    kind = lax.broadcasted_iota(jnp.int32, (8, 2 * nz), 0)
    lane = lax.broadcasted_iota(jnp.int32, (8, 2 * nz), 1)
    at = lane - nz
    add = (kind == 0) & (lane < nz)
    add |= (kind == 1) & (at == 0)
    add |= (kind == 2) & (at >= 0) & (at <= 1)
    add |= (kind == 3) & (at >= nz - 2)
    add |= (kind == 4) & (at == nz - 1)
    return twice(add)


def face_weights(cy):
    row = lax.broadcasted_iota(jnp.int32, (128, 128), 0)
    col = lax.broadcasted_iota(jnp.int32, (128, 128), 1)
    same = row // cy == col // cy
    r, c = row % cy, col % cy
    return [
        twice(same & (r <= c)),
        twice(same),
        twice(same & (jnp.abs(r - c) <= 2)),
        twice(same & (c + cy - r <= 2)),
        twice(same & (r + cy - c <= 2)),
    ]


def y_prefix(piece, start):
    ny, nz = piece.shape
    row = lax.broadcasted_iota(jnp.int32, (1, 8, nz), 1)
    c = piece.reshape(ny // 8, 8, nz)
    for step in (1, 2, 4):
        c = c + jnp.where(row >= step, pltpu.roll(c, step, 1), 0.0)
    out = []
    for k in range(ny // 8):
        out.append(c[k] + start)
        start = out[-1][7:8]
    return jnp.concatenate(out, axis=0)


def y_box(tall, slot, piece, before, after):
    ny = piece.shape[0]
    tall[slot, pl.ds(8, ny), :] = piece
    tall[slot, pl.ds(6, 1), :] = before[0]
    tall[slot, pl.ds(7, 1), :] = before[1]
    tall[slot, pl.ds(8 + ny, 1), :] = after[0]
    tall[slot, pl.ds(9 + ny, 1), :] = after[1]
    total = piece
    for d in (6, 7, 9, 10):
        total = total + tall[slot, pl.ds(d, ny), :]
    return total


class Exchange:
    def __init__(self, send, recv):
        self.send, self.recv, self.count = send, recv, 0

    def start(self, shifts, src, dst, step=0):
        at = self.count
        self.count += 1
        device, sends, receives = {}, True, True
        for axis, d in shifts.items():
            n, me = lax.axis_size(axis), lax.axis_index(axis)
            device[axis] = lax.rem(me + d + n, n)
            sends = (me + d >= 0) & (me + d < n) & sends
            receives = (me - d >= 0) & (me - d < n) & receives
            if step:
                sends &= lax.rem(me, 2 * step) == step - 1
                receives &= lax.rem(me - d + n, 2 * step) == step - 1
        copy = pltpu.make_async_remote_copy(
            src_ref=src,
            dst_ref=dst,
            send_sem=self.send.at[at],
            recv_sem=self.recv.at[at],
            device_id=device,
            device_id_type=MESH,
        )
        pl.when(sends)(copy.start)
        return sends, receives, copy


def arrived(copies):
    for _, receives, copy in copies:
        pl.when(receives)(copy.wait_recv)


def sent(copies):
    for sends, _, copy in copies:
        pl.when(sends)(copy.wait_send)


def total_of(ref, count=None):
    total = ref[0]
    for d in range(1, count or ref.shape[0]):
        total = total + ref[d]
    return total


def doublings(n):
    return [1 << k for k in range((n - 1).bit_length())]


def sides(n):
    return ((0, 1), (1, -1)) if n > 1 else ()


def exchange_kernel(
    cx, cy, cz, v_hbm,
    yp_out, yb_out, xk_out, xe_out, zk_out,
    v, g, xsrc, ysrc, zraw, zsrc, xzp, xzb,
    yc, yh, zyc, zyh, xc, xh, zc, zh, xzc, xzh, q, zfw, qfw, gyc, gyh, tall, w, fw,
    load, send, recv,
):
    nx, ny, nz = (lax.axis_size(a) for a in ("gx", "gy", "gz"))
    chunk = PLANES * cy
    steps = cx // PLANES
    arows = cx * cy // 128
    per = arows // steps

    def load_of(i):
        at = pl.ds(pl.multiple_of(i * chunk, chunk), chunk)
        return pltpu.make_async_copy(v_hbm.at[at], v.at[at], load.at[i])

    for i in range(steps):
        load_of(i).start()
    for ref in (yc, yh, zyc, zyh, xc, xh, zc, zh, xzc, xzh, q):
        ref[...] = jnp.zeros_like(ref)
    barrier = pltpu.get_barrier_semaphore()
    near = [{"gy": d} for d in range(1, ny)] + [{"gx": d} for d in range(1, nx)]
    near += [{"gz": d} for d in range(1, nz)]
    near += [{"gx": d, "gz": e} for _, d in sides(nx) for _, e in sides(nz) if d > 0]
    peers = 0
    for shifts in near:
        for sign in (1, -1):
            there, device = True, {}
            for axis, d in shifts.items():
                to, n = lax.axis_index(axis) + sign * d, lax.axis_size(axis)
                there = (to >= 0) & (to < n) & there
                device[axis] = lax.rem(to + n, n)

            @pl.when(there)
            def _():
                pl.semaphore_signal(barrier, inc=1, device_id=device, device_id_type=MESH)

            peers = peers + there.astype(jnp.int32)

    w[...] = jnp.concatenate(z_weights(cz), axis=1)
    for k, weight in enumerate(face_weights(cy)):
        fw[k] = weight

    def sources(i, xsum):
        load_of(i).wait()
        base = pl.multiple_of(i * chunk, chunk)
        here = pl.ds(pl.multiple_of(i * PLANES, PLANES), PLANES)
        for p in range(PLANES):
            xsum = xsum + v[pl.ds(base + p * cy, cy), :]
        ysrc[0, here, :] = jnp.sum(v[pl.ds(base, chunk), :].reshape(PLANES, cy, cz), axis=1)
        for k, j in ((1, cy - 2), (2, cy - 1), (3, 0), (4, 1)):
            ysrc[k, here, :] = v[pl.ds(base + j, PLANES, stride=cy), :]
        for b in range(per):
            t = v[pl.ds(base + b * 128, 128), :].T
            row = pl.ds(i * per + b, 1)
            zraw[0, row, :] = jnp.sum(t, axis=0, keepdims=True)
            for k, z in ((1, cz - 2), (2, cz - 1), (3, 0), (4, 1)):
                zraw[k, row, :] = t[z : z + 1]
        return xsum

    xsum = lax.fori_loop(0, steps, sources, jnp.zeros((cy, cz), F32))
    xsrc[0] = xsum
    pl.semaphore_wait(barrier, peers)

    ex = Exchange(send, recv)
    to_y = []
    for s, d in sides(ny):
        to_y.append(ex.start({"gy": d}, ysrc.at[pl.ds(1 + 2 * s, 2)], yh.at[pl.ds(2 * s, 2)]))
        to_y.append(ex.start({"gy": d}, zraw.at[pl.ds(1, 4)], zyh.at[s]))
    for d in range(1, ny):
        to_y.append(ex.start({"gy": d}, ysrc.at[0], yc.at[d - 1]))
        to_y.append(ex.start({"gy": d}, zraw.at[0], zyc.at[d - 1]))

    def along_z(i):
        at = pl.ds(pl.multiple_of(i * chunk, chunk), chunk)
        g[at, :] = dot(split(v[at, :], 1), w[...])

    early = EARLY
    pl.loop(0, early)(along_z)
    w_low, w_one, w_band, w_down, w_up = (fw[k] for k in range(5))
    arrived(to_y)

    ycar = total_of(yc)
    zsrc[0] = dot(split(zraw[0], 1), w_low) + dot(split(total_of(zyc), 1), w_one)

    def flat(a):
        return split(a.reshape(4 * arows, 128), 1)

    faces = dot(flat(zraw[pl.ds(1, 4)]), w_band)
    faces = faces + dot(flat(zyh[0]), w_down) + dot(flat(zyh[1]), w_up)
    zsrc[pl.ds(1, 4)] = faces.reshape(4, arows, 128)
    line = jnp.sum(zsrc[0], axis=0, keepdims=True)
    whole = line
    for p in range(1, 128 // cy):
        whole = whole + pltpu.roll(line, p * cy, 1)
    xzp[...] = jnp.broadcast_to(whole, (8, 128))
    for s, a in ((0, arows - 1), (1, 0)):
        for k in range(4):
            xzb[2 * s + k // 2, pl.ds(k % 2, 1), :] = zsrc[1 + k, pl.ds(a, 1), :]

    steps_z = doublings(nz)

    def pass_on(k, src, slots):
        step = steps_z[k]
        return [ex.start({"gz": d}, src, slots.at[k], step) for d in range(1, step + 1)]

    lines = [ex.start({"gx": d}, xzp, xzc.at[d - 1]) for d in range(1, nx)]
    rest, carries, ends = [], [], []
    if steps_z:
        carries.append(pass_on(0, zsrc.at[0], zc))
    for s, d in sides(nz)[::-1]:
        rest.append(ex.start({"gz": d}, zsrc.at[pl.ds(1 + 2 * s, 2)], zh.at[pl.ds(2 * s, 2)]))
    xsrc[0] = y_prefix(xsum, jnp.sum(ycar, axis=0, keepdims=True))
    for k, x in enumerate((cx - 2, cx - 1, 0, 1)):
        rows = [yh[b, pl.ds(x, 1), :] for b in range(4)]
        xsrc[1 + k] = y_box(tall, k, v[pl.ds(x * cy, cy), :], rows[:2], rows[2:])
    for s, d in sides(nx)[::-1]:
        rest.append(ex.start({"gx": d}, xsrc.at[pl.ds(1 + 2 * s, 2)], xh.at[pl.ds(2 * s, 2)]))
    for d in range(1, nx):
        rest.append(ex.start({"gx": d}, xsrc.at[0], xc.at[d - 1]))
    for s, d in sides(nx):
        for t, e in sides(nz):
            at = 2 * s + t
            rest.append(ex.start({"gx": d, "gz": e}, xzb.at[at], xzh.at[at]))

    def forward_carry(k):
        arrived(carries[-1])
        zfw[k] = zsrc[0] + total_of(zc, k)
        carries.append(pass_on(k, zfw.at[k], zc))

    def forward_line():
        arrived(lines)
        qfw[0] = total_of(xzc)
        ends.append([ex.start({"gz": d}, qfw.at[0], q.at[d - 1]) for d in range(1, nz)])

    gyc[...] = dot(split(ycar, 1), w[:, pl.ds(0, cz)])
    gyh[...] = dot(split(yh[...].reshape(4 * cx, cz), 1), w[:, pl.ds(cz, cz)]).reshape(4, cx, cz)

    def along_y(i):
        here = pl.ds(pl.multiple_of(i * PLANES, PLANES), PLANES)
        starts = gyc[here, :]
        beyond = [gyh[k, here, :] for k in range(4)]
        for p in range(PLANES):
            at = pl.ds(pl.multiple_of(i * chunk, chunk) + p * cy, cy)
            rows = [e[p : p + 1] for e in beyond]
            yp_out[at, :] = y_prefix(g[at, pl.ds(0, cz)], starts[p : p + 1])
            yb_out[at, :] = y_box(tall, p % 4, g[at, pl.ds(cz, cz)], rows[:2], rows[2:])

    work = [functools.partial(pl.loop(early, steps), along_z)]
    work += [functools.partial(pl.loop(i, i + 2), along_y) for i in range(0, steps, 2)]
    jobs = [forward_line] + [functools.partial(forward_carry, k) for k in range(1, len(steps_z))]
    while work or jobs:
        if work:
            work.pop(0)()
        if jobs and len(work) < 4:
            jobs.pop(0)()

    arrived(rest + sum(carries[-1:] + ends[-1:], []))
    xk_out[0] = total_of(xc)
    xk_out[pl.ds(1, 4)] = xh[...]
    zero = jnp.zeros((8, 128), F32)
    row = lax.broadcasted_iota(jnp.int32, (8, 128), 0)
    xe_out[0] = jnp.where(row == 0, total_of(q), zero)
    for s in range(2):
        low, high = pltpu.roll(xzh[2 * s], 1, 0), pltpu.roll(xzh[2 * s + 1], 3, 0)
        inside = jnp.where((row == 1) | (row == 2), low, zero)
        xe_out[1 + s] = jnp.where((row == 3) | (row == 4), high, inside)
    zk_out[...] = jnp.zeros_like(zk_out)
    zk_out[0, pl.ds(0, arows), :] = total_of(zc)
    zk_out[pl.ds(1, 4), pl.ds(0, arows), :] = zh[...]
    sent(to_y + lines + rest + sum(carries + ends, []))


def final_kernel(
    cx, cy, cz, scale, yp, yb, xk, xe, zk, prefix_hbm, box_hbm, mm, prefix, box, psem, bsem
):
    chunk = PLANES * cy
    steps = cx // PLANES
    arows = cx * cy // 128
    per = arows // steps
    pad = zk.shape[0] // 8
    box_scale = F32(1.0 / math.sqrt(125.0))
    edge = edge_weights(cz)
    lower, band = z_weights(cz)

    outer = dot_t(split(jnp.concatenate([xe[0], xe[1], xe[2]], axis=1), 0), edge)
    running = dot(split(xk[0], 1), lower) + outer[:cy, :cz]
    halo = dot(split(xk[pl.ds(1, 4)].reshape(4 * cy, cz), 1), band) + outer[128 : 128 + 4 * cy, cz:]
    halo = [halo[k * cy : (k + 1) * cy] for k in range(4)]

    def put(src, dst, sem):
        copy = pltpu.make_async_copy(src, dst, sem)
        copy.start()
        return copy

    copies = []
    window = halo[:2]
    for i in range(steps):
        slot = i % 2
        tiles = [zk[pl.ds(i * per + b, 8, stride=pad), :] for b in range(per)]
        mm[slot] = dot_t(split(jnp.concatenate(tiles, axis=1), 0), edge)
        for p in range(PLANES):
            x = i * PLANES + p
            at, here = pl.ds(x * cy, cy), pl.ds(p * cy, cy)
            running = running + (yp[at, :] + mm[slot, here, pl.ds(0, cz)])
            prefix[at, :] = running * F32(scale)
            window.append(yb[at, :] + mm[slot, here, pl.ds(cz, cz)])
            if len(window) == 5:
                total = (window[0] + window[1]) + (window[2] + window[3]) + window[4]
                box[pl.ds((x - 2) * cy, cy), :] = total * box_scale
                window = window[1:]
        at = pl.ds(i * chunk, chunk)
        copies.append(put(prefix.at[at], prefix_hbm.at[at], psem.at[i]))
        first = max(i * PLANES - 2, 0)
        at = pl.ds(first * cy, ((i + 1) * PLANES - 2 - first) * cy)
        copies.append(put(box.at[at], box_hbm.at[at], bsem.at[i]))
    for k in (2, 3):
        window.append(halo[k])
        total = (window[0] + window[1]) + (window[2] + window[3]) + window[4]
        box[pl.ds((cx - 4 + k) * cy, cy), :] = total * box_scale
        window = window[1:]
    at = pl.ds((cx - 2) * cy, 2 * cy)
    copies.append(put(box.at[at], box_hbm.at[at], bsem.at[steps]))
    for copy in copies:
        copy.wait()


def per_device(volume):
    cx, cy, cz = volume.shape
    nx, ny, nz = (lax.axis_size(a) for a in ("gx", "gy", "gz"))
    steps = cx // PLANES
    rows = cx * cy
    arows = rows // 128
    lx, ly = (max(n - 1, 1) for n in (nx, ny))
    lz = max(len(doublings(nz)), 1)
    copies = 4 + 2 * ly + 2 + 2 + lx + 4 + lx + 2 * nz
    vmem = pl.BlockSpec(memory_space=pltpu.VMEM)
    hbm = pl.BlockSpec(memory_space=pltpu.HBM)
    flat = pltpu.with_memory_space_constraint(volume.reshape(rows, cz), pltpu.HBM)

    outs = [(rows, cz), (rows, cz), (5, cy, cz), (3, 8, 128), (8, arows + 8, 128)]
    buffers = [
        (rows, cz), (rows, 2 * cz), (5, cy, cz), (5, cx, cz),
        (5, arows, 128), (5, arows, 128), (8, 128), (4, 8, 128),
        (ly, cx, cz), (4, cx, cz), (ly, arows, 128), (2, 4, arows, 128),
        (lx, cy, cz), (4, cy, cz), (lz, arows, 128), (4, arows, 128),
        (lx, 8, 128), (4, 8, 128), (max(nz - 1, 1), 8, 128), (lz, arows, 128), (1, 8, 128), (cx, cz), (4, cx, cz), (4, cy + 16, cz),
    ]
    yp, yb, xk, xe, zk = pl.pallas_call(
        functools.partial(exchange_kernel, cx, cy, cz),
        in_specs=[hbm],
        out_specs=[vmem] * len(outs),
        out_shape=[pltpu.VMEM(s, F32) for s in outs],
        scratch_shapes=[pltpu.VMEM(s, F32) for s in buffers]
        + [
            pltpu.VMEM((2 * cz, 2 * cz), BF16),
            pltpu.VMEM((5, 256, 128), BF16),
            pltpu.SemaphoreType.DMA((steps,)),
            pltpu.SemaphoreType.DMA((copies,)),
            pltpu.SemaphoreType.DMA((copies,)),
        ],
        compiler_params=pltpu.CompilerParams(
            collective_id=0, has_side_effects=True, vmem_limit_bytes=40 * 1024 * 1024
        ),
    )(flat)

    scale = 1.0 / math.sqrt(cx * nx * cy * ny * cz * nz)
    prefix, box = pl.pallas_call(
        functools.partial(final_kernel, cx, cy, cz, scale),
        in_specs=[vmem] * 5,
        out_specs=[hbm] * 2,
        out_shape=[jax.ShapeDtypeStruct((rows, cz), F32)] * 2,
        scratch_shapes=[
            pltpu.VMEM((2, PLANES * cy, 2 * cz), F32),
            pltpu.VMEM((rows, cz), F32),
            pltpu.VMEM((rows, cz), F32),
            pltpu.SemaphoreType.DMA((steps,)),
            pltpu.SemaphoreType.DMA((steps + 1,)),
        ],
        compiler_params=pltpu.CompilerParams(vmem_limit_bytes=40 * 1024 * 1024),
    )(yp, yb, xk, xe, zk.reshape(8 * (arows + 8), 128))
    return prefix.reshape(cx, cy, cz), box.reshape(cx, cy, cz)


def solution(mesh):
    return jax.shard_map(
        per_device,
        mesh=mesh,
        in_specs=(P("gx", "gy", "gz"),),
        out_specs=(P("gx", "gy", "gz"), P("gx", "gy", "gz")),
        check_vma=False,
    )
```
